256 devices in a mesh: out: 32 (over z, y), inp: 8 (over x, core).
Axes of the slice: x: 4, y: 4, z: 8, core: 2. Of those that a mesh axis runs over, the one named last changes fastest.
Arguments:
- weight: float32 [32, 512, 13824], P(None, 'out', 'inp'), may hold values from -6 to 6
- gradient: bfloat16 [32, 512, 13824], P(None, 'out', 'inp'), may hold values from -60 to 60
- momentum: bfloat16 [32, 512, 13824], P(None, 'out', 'inp'), may hold values from -6 to 6
Outputs:
- weight_next: float32 [32, 512, 13824], P(None, 'out', 'inp')
- momentum_next: bfloat16 [32, 512, 13824], P(None, 'out', 'inp')
The draws below stay inside these ranges and needn't reach their ends.
All inputs are finite; a program needn't handle non-finite values.
Results may differ from the reference program's by a relative error of at most 0.0039.
Values may be sent and summed in bfloat16 or wider, within the bound.
A program may use at most 64 MiB of HBM per device.

```python
import math
import jax
import jax.numpy as jnp
from jax import lax

OUTC = 512
ITERS = 5
COLS = 13824
KERNELS = 32


def draw_gradient(key, part):
    keys = jax.random.split(key, 3)
    row_scale = jnp.exp(jax.random.uniform(keys[1], (KERNELS, OUTC, 1), jnp.float32) * math.log(10.0))
    col_scale = jnp.exp(jax.random.uniform(keys[2], (KERNELS, 1, COLS), jnp.float32) * math.log(10.0))
    values = jnp.clip(jax.random.normal(keys[0], (KERNELS, OUTC, COLS), jnp.float32), -6.0, 6.0)
    result = values * row_scale * col_scale / 10.0
    return result.astype(jnp.bfloat16)


def level_of(own_key, shape, cuts, least, top_value):
    gain = 1.0
    for dim, parts in cuts:
        draws = jax.random.uniform(jax.random.fold_in(jax.random.fold_in(own_key, 6), dim), (parts,), jnp.float32, least / len(cuts), top_value / len(cuts))
        gain = gain * jnp.repeat(jnp.exp(draws), shape[dim] // parts).reshape((-1,) + (1,) * (len(shape) - 1 - dim))
    return gain


def normal_values(key, extent, width, most, cuts=(), kind=jnp.bfloat16):
    values = jax.random.normal(key, extent, jnp.float32) * width
    if len(cuts) > 0:
        values = level_of(key, extent, cuts, -0.22, 0.18) * values
    return jnp.clip(values, min=-most, max=most).astype(kind)


def setup_inputs(seed: int = 0) -> dict:
    key_list = jax.random.split(jax.random.key(seed), 4)
    weight = normal_values(key_list[0], (KERNELS, OUTC, COLS), 1.0, 6.0, ((1, 32), (2, 8)), jnp.float32)
    gradient = draw_gradient(jax.random.fold_in(key_list[3], 71), 0)
    momentum = normal_values(key_list[2], (KERNELS, OUTC, COLS), 1.0, 6.0, ((1, 32), (2, 8)))
    return {"weight": weight, "gradient": gradient, "momentum": momentum}


BETA = 0.95
EPSILON = 1e-06
COEF_A = 3.4445
COEF_B = -4.775
COEF_C = 2.0315

def mult(former, latter):
    return jnp.dot(former, latter, precision=lax.Precision.HIGHEST)

def single_kernel(item):
    weights, grads, moments = item
    moment = BETA * moments.astype(jnp.float32) + grads.astype(jnp.float32)
    source = (grads.astype(jnp.float32) + BETA * moment).astype(jnp.bfloat16)
    gram = jnp.dot(source, source.T, preferred_element_type=jnp.float32)
    widened = source.astype(jnp.float32)
    scale2 = jnp.sum(widened * widened) + EPSILON
    current = gram / scale2
    transform = jnp.eye(OUTC, dtype=jnp.float32)
    for sweep in range(ITERS):
        poly_part = COEF_B * current + COEF_C * mult(current, current)
        transform = COEF_A * transform + mult(poly_part, transform)
        halfway = COEF_A * current + mult(poly_part, current)
        current = COEF_A * halfway + mult(halfway, poly_part)
    factor = (transform / jnp.sqrt(scale2)).astype(jnp.bfloat16)
    orthogonal = jnp.dot(factor, source, preferred_element_type=jnp.float32)
    update = (0.2 * math.sqrt(COLS) * orthogonal).astype(jnp.bfloat16)
    weight_next = 0.9 * weights - 0.5 * update.astype(jnp.float32)
    return (weight_next, moment.astype(jnp.bfloat16))

def reference(weight, gradient, momentum):
    weight_next, momentum_next = lax.map(single_kernel, (weight, gradient, momentum))
    return (weight_next, momentum_next)
```

```python
import functools
import math

import jax
import jax.numpy as jnp
from jax import lax
from jax.experimental import pallas as pl
from jax.experimental.pallas import tpu as pltpu
from jax.sharding import PartitionSpec as P

ITERS = 5
COLS = 13824
BETA = 0.95
EPSILON = 1e-06
COEF_A = 3.4445
COEF_B = -4.775
COEF_C = 2.0315

MESH = pl.DeviceIdType.MESH
BF16 = jnp.bfloat16
F32 = jnp.float32

ZS, YS, INP = 8, 4, 8
OUT = ZS * YS
BATCHES = 2
ROWS = 512
BLOCK = 16
WIDTH = 1792
HALF = WIDTH // BATCHES
GROUP = INP * BATCHES
PIECES = [(i, j) for i in range(4) for j in range(i, 4)]
SLICE = 128 * len(PIECES) // GROUP


def dot(a, b):
    return lax.dot_general(a, b, (((1,), (0,)), ((), ())), preferred_element_type=F32)


def dot_t(a, b):
    return lax.dot_general(a, b, (((1,), (1,)), ((), ())), preferred_element_type=F32)


def split(x):
    high = x.astype(BF16)
    return high, (x - high.astype(F32)).astype(BF16)


def product(a, b):
    return dot(a[0][...], b[0][...]) + dot(a[0][...], b[1][...]) + dot(a[1][...], b[0][...])


def put(pair, x):
    high, low = split(x)
    pair[0][...] = high
    pair[1][...] = low


def kernel(
    src, ret, held, upd, packed, slots, own, full, rh, rl, qh, ql, mh, ml, yh, yl,
    f_send, f_recv, b_send, b_recv, r_send, r_recv, g_send, g_recv, local,
):
    me = lax.axis_index("out")
    inp = lax.axis_index("inp")
    z, y = me // YS, lax.rem(me, YS)
    team, seat = me // BATCHES, lax.rem(me, BATCHES)
    rank = seat * INP + inp

    def partner(i):
        at = lax.rem(i, OUT) + i // OUT
        t = at // YS
        step = jnp.where(lax.rem(t, 2) == 1, (t + 1) // 2, ZS - t // 2)
        return lax.rem(z + step, ZS) * YS + lax.rem(y + lax.rem(at, YS), YS), at

    def mate(j):
        other = lax.rem(rank + j, GROUP)
        return (team * BATCHES + other // INP, lax.rem(other, INP)), other

    barrier = pltpu.get_barrier_semaphore()

    def greet(i, c):
        pl.semaphore_signal(barrier, inc=1, device_id=(partner(i)[0], inp), device_id_type=MESH)
        return c

    def greet_mate(j, c):
        pl.semaphore_signal(barrier, inc=1, device_id=mate(j)[0], device_id_type=MESH)
        return c

    lax.fori_loop(YS, YS + OUT - 1, greet, 0)
    lax.fori_loop(1, GROUP, greet_mate, 0)
    pl.semaphore_wait(barrier, OUT - 1 + GROUP - 1)

    my_rows = pl.ds(pl.multiple_of(me * BLOCK, BLOCK), BLOCK)
    my_cols = pl.ds(pl.multiple_of(seat * HALF, 128), HALF)

    def forward(b, i):
        dest, at = partner(i)
        cols = pl.ds(pl.multiple_of(lax.rem(dest, BATCHES) * HALF, 128), HALF)
        return pltpu.make_async_remote_copy(
            src_ref=src.at[dest // BATCHES * BATCHES + b, :, cols],
            dst_ref=held.at[b, my_rows],
            send_sem=f_send.at[b, at],
            recv_sem=f_recv.at[b, at],
            device_id=(dest, inp),
            device_id_type=MESH,
        )

    def backward(b, i):
        dest, at = partner(i)
        return pltpu.make_async_remote_copy(
            src_ref=upd.at[b, pl.ds(pl.multiple_of(dest * BLOCK, BLOCK), BLOCK)],
            dst_ref=ret.at[team * BATCHES + b, :, my_cols],
            send_sem=b_send.at[b, at],
            recv_sem=b_recv.at[b, at],
            device_id=(dest, inp),
            device_id_type=MESH,
        )

    def scatter(b, j):
        device, other = mate(j)
        return pltpu.make_async_remote_copy(
            src_ref=packed.at[b, pl.ds(pl.multiple_of(other * SLICE, 16), SLICE)],
            dst_ref=slots.at[b, j],
            send_sem=r_send.at[b, j],
            recv_sem=r_recv.at[b, j],
            device_id=device,
            device_id_type=MESH,
        )

    def gather(b, j):
        device, _ = mate(j)
        return pltpu.make_async_remote_copy(
            src_ref=own.at[b],
            dst_ref=full.at[b, pl.ds(pl.multiple_of(rank * SLICE, 16), SLICE)],
            send_sem=g_send.at[b, j],
            recv_sem=g_recv.at[b, j],
            device_id=device,
            device_id_type=MESH,
        )

    def start_all(copy, b, low, high):
        def body(i, c):
            copy(b, i).start()
            return c

        lax.fori_loop(low, high, body, 0)

    def wait_recv_all(copy, b, low, high):
        def body(i, c):
            copy(b, i).wait_recv()
            return c

        lax.fori_loop(low, high, body, 0)

    def wait_send_all(copy, b, low, high):
        def body(i, c):
            copy(b, i).wait_send()
            return c

        lax.fori_loop(low, high, body, 0)

    def keep_forward(b):
        return pltpu.make_async_copy(
            src.at[team * BATCHES + b, :, my_cols], held.at[b, my_rows], local.at[0, b]
        )

    def keep_backward(b):
        return pltpu.make_async_copy(
            upd.at[b, my_rows], ret.at[team * BATCHES + b, :, my_cols], local.at[1, b]
        )

    PEERS = (YS, YS + OUT - 1)
    MATES = (1, GROUP)

    for b in range(BATCHES):
        start_all(forward, b, *PEERS)
        keep_forward(b).start()

    def gram(b):
        keep_forward(b).wait()
        wait_recv_all(forward, b, *PEERS)
        top = dot_t(held[b, 0:256, :], held[b]).astype(BF16)
        low = dot_t(held[b, 256:512, :], held[b, 256:512, :]).astype(BF16)
        for n, (i, j) in enumerate(PIECES):
            part = top[128 * i : 128 * i + 128, 128 * j : 128 * j + 128] if i < 2 else low[128 * i - 256 : 128 * i - 128, 128 * j - 256 : 128 * j - 128]
            packed[b, 128 * n : 128 * n + 128, :] = part
        start_all(scatter, b, *MATES)

    def reduce(b):
        total = packed[b, pl.ds(pl.multiple_of(rank * SLICE, 16), SLICE), :].astype(F32)
        wait_recv_all(scatter, b, *MATES)
        for j in range(1, GROUP):
            total = total + slots[b, j].astype(F32)
        own[b] = total
        full[b, pl.ds(pl.multiple_of(rank * SLICE, 16), SLICE), :] = total
        start_all(gather, b, *MATES)

    R, Q, M, Y = (rh, rl), (qh, ql), (mh, ml), (yh, yl)

    def eye(x):
        rows = lax.broadcasted_iota(jnp.int32, x.shape, 0)
        cols = lax.broadcasted_iota(jnp.int32, x.shape, 1)
        return rows == cols

    def poly():
        m = COEF_C * product(R, R) + COEF_B * (rh[...].astype(F32) + rl[...].astype(F32))
        put(M, m + jnp.where(eye(m), COEF_A, 0.0))

    def advance():
        put(Y, product(M, R))
        put(R, product(Y, M))

    def finish(b):
        wait_recv_all(gather, b, *MATES)
        trace = jnp.zeros((), F32)
        for n, (i, j) in enumerate(PIECES):
            if i == j:
                part = full[b, 128 * n : 128 * n + 128, :]
                trace = trace + jnp.sum(jnp.where(eye(part), part, 0.0))
        scale2 = trace + EPSILON
        inverse = 1.0 / jnp.full((128, 128), scale2, F32)
        for n, (i, j) in enumerate(PIECES):
            part = full[b, 128 * n : 128 * n + 128, :] * inverse
            high, low = split(part)
            rows, cols = slice(128 * i, 128 * i + 128), slice(128 * j, 128 * j + 128)
            rh[rows, cols] = high
            rl[rows, cols] = low
            if i != j:
                high, low = split(part.T)
                rh[cols, rows] = high
                rl[cols, rows] = low
        poly()
        qh[...] = mh[...]
        ql[...] = ml[...]
        advance()

        def sweep(i, c):
            poly()
            put(Q, product(Q, M))
            advance()
            pl.when(jnp.logical_and(b == 0, i == 1))(lambda: gram(1))
            pl.when(jnp.logical_and(b == 0, i == 2))(lambda: reduce(1))
            return c

        lax.fori_loop(0, ITERS - 2, sweep, 0)
        poly()
        root = jnp.sqrt(jnp.full((ROWS, ROWS), scale2, F32))
        factor = (product(Q, M) / root).astype(BF16)
        upd[b] = (0.2 * math.sqrt(COLS) * dot(factor, held[b])).astype(BF16)
        start_all(backward, b, *PEERS)
        keep_backward(b).start()

    gram(0)
    reduce(0)

    def batch(b, c):
        finish(b)
        return c

    lax.fori_loop(0, BATCHES, batch, 0)
    for b in range(BATCHES):
        keep_backward(b).wait()
        wait_send_all(forward, b, *PEERS)
        wait_send_all(scatter, b, *MATES)
        wait_send_all(gather, b, *MATES)
        wait_send_all(backward, b, *PEERS)
        wait_recv_all(backward, b, *PEERS)


def exchange(source):
    matrix = pltpu.VMEM((ROWS, ROWS), BF16)
    dma = pltpu.SemaphoreType.DMA
    return pl.pallas_call(
        kernel,
        out_shape=jax.ShapeDtypeStruct((OUT, BLOCK, WIDTH), BF16),
        in_specs=[pl.BlockSpec(memory_space=pltpu.VMEM)],
        out_specs=pl.BlockSpec(memory_space=pltpu.VMEM),
        scratch_shapes=[
            pltpu.VMEM((BATCHES, ROWS, HALF), BF16),
            pltpu.VMEM((BATCHES, ROWS, HALF), BF16),
            pltpu.VMEM((BATCHES, 128 * len(PIECES), 128), BF16),
            pltpu.VMEM((BATCHES, GROUP, SLICE, 128), BF16),
            pltpu.VMEM((BATCHES, SLICE, 128), F32),
            pltpu.VMEM((BATCHES, 128 * len(PIECES), 128), F32),
            *[matrix] * 8,
            dma((BATCHES, OUT)), dma((BATCHES, OUT)), dma((BATCHES, OUT)), dma((BATCHES, OUT)),
            dma((BATCHES, GROUP)), dma((BATCHES, GROUP)), dma((BATCHES, GROUP)), dma((BATCHES, GROUP)),
            dma((2, BATCHES)),
        ],
        compiler_params=pltpu.CompilerParams(collective_id=0, has_side_effects=True),
        name="muon",
    )(source)


def on_device(weight, gradient, momentum):
    moment = BETA * momentum.astype(F32) + gradient.astype(F32)
    source = (gradient.astype(F32) + BETA * moment).astype(BF16)
    padded = jnp.pad(source, ((0, 0), (0, 0), (0, WIDTH - source.shape[2])))
    returned = exchange(padded)[:, :, : source.shape[2]]
    weight_next = 0.9 * weight - 0.5 * returned.astype(F32)
    return (weight_next, moment.astype(BF16))


def solution(mesh):
    spec = P(None, "out", "inp")
    return jax.shard_map(
        on_device, mesh=mesh, in_specs=(spec, spec, spec), out_specs=(spec, spec), check_vma=False
    )
```

```python
import functools
import math

import jax
import jax.numpy as jnp
from jax import lax
from jax.experimental import pallas as pl
from jax.experimental.pallas import tpu as pltpu
from jax.sharding import PartitionSpec as P

ITERS = 5
COLS = 13824
BETA = 0.95
EPSILON = 1e-06
COEF_A = 3.4445
COEF_B = -4.775
COEF_C = 2.0315

MESH = pl.DeviceIdType.MESH
BF16 = jnp.bfloat16
F32 = jnp.float32

ZS, YS, INP = 8, 4, 8
OUT = ZS * YS
BATCHES = 2
ROWS = 512
BLOCK = 16
WIDTH = 1792
HALF = WIDTH // BATCHES
GROUP = INP // 2 * BATCHES
PIECES = [(i, j) for i in range(4) for j in range(i, 4)]
TALL = 128 * len(PIECES)
SLICE = TALL // GROUP
VMEM_LIMIT = 50 * 2**20


def dot(a, b):
    return lax.dot_general(a, b, (((1,), (0,)), ((), ())), preferred_element_type=F32)


def dot_t(a, b):
    return lax.dot_general(a, b, (((1,), (1,)), ((), ())), preferred_element_type=F32)


def split(x):
    high = x.astype(BF16)
    return high, (x - high.astype(F32)).astype(BF16)


def product(a, b):
    return dot(a[0][...], b[0][...]) + dot(a[0][...], b[1][...]) + dot(a[1][...], b[0][...])


def put(pair, x):
    high, low = split(x)
    pair[0][...] = high
    pair[1][...] = low


def kernel(
    grad, mom, ret, mom_next, src, held, upd, packed, slots, own, full, factor,
    rh, rl, qh, ql, mh, ml, yh, yl, grad_in, mom_in, mom_out,
    f_send, f_recv, b_send, b_recv, r_send, r_recv, g_send, g_recv, local, load, store,
):
    me = lax.axis_index("out")
    inp = lax.axis_index("inp")
    z, y = me // YS, lax.rem(me, YS)
    team, seat = me // BATCHES, lax.rem(me, BATCHES)
    x, core = inp // 2, lax.rem(inp, 2)
    rank = seat * (INP // 2) + x
    mine = team * BATCHES + core
    width = grad.shape[2]

    loads = [
        pltpu.make_async_copy(grad, grad_in, load.at[0]),
        pltpu.make_async_copy(mom, mom_in, load.at[1]),
    ]
    for copy in loads:
        copy.start()

    def partner(i):
        at = lax.rem(i, OUT) + i // OUT
        t = at // YS
        step = jnp.where(lax.rem(t, 2) == 1, (t + 1) // 2, ZS - t // 2)
        return lax.rem(z + step, ZS) * YS + lax.rem(y + lax.rem(at, YS), YS)

    def mate(j):
        other = lax.rem(rank + j, GROUP)
        return (team * BATCHES + other // (INP // 2), 2 * lax.rem(other, INP // 2) + core), other

    barrier = pltpu.get_barrier_semaphore()

    def greet(i, c):
        dest = lax.rem(me + i, OUT)
        for other in range(2):
            pl.semaphore_signal(barrier, inc=1, device_id=(dest, 2 * x + other), device_id_type=MESH)
        return c

    def greet_mate(j, c):
        pl.semaphore_signal(barrier, inc=1, device_id=mate(j)[0], device_id_type=MESH)
        return c

    lax.fori_loop(1, OUT, greet, 0)
    lax.fori_loop(1, GROUP, greet_mate, 0)
    pl.semaphore_signal(barrier, inc=1, device_id=(me, 2 * x + 1 - core), device_id_type=MESH)

    for copy in loads:
        copy.wait()

    def elementwise(k, c):
        g = grad_in[k].astype(F32)
        moment = BETA * mom_in[k].astype(F32) + g
        mom_out[k] = moment.astype(BF16)
        src[k, :, 0:width] = (g + BETA * moment).astype(BF16)
        src[k, :, width:WIDTH] = jnp.zeros((BLOCK, WIDTH - width), BF16)
        return c

    lax.fori_loop(0, OUT, elementwise, 0)
    keep_moment = pltpu.make_async_copy(mom_out, mom_next, store)
    keep_moment.start()
    pl.semaphore_wait(barrier, 2 * (OUT - 1) + GROUP - 1 + 1)

    def block(dest):
        return pl.ds(pl.multiple_of(dest * BLOCK, BLOCK), BLOCK)

    def half(which):
        return pl.ds(pl.multiple_of(which * HALF, 128), HALF)

    def place(dest):
        return lax.rem(dest // YS - z + ZS, ZS) * YS + lax.rem(lax.rem(dest, YS) - y + YS, YS)

    def forward(b, dest):
        return pltpu.make_async_remote_copy(
            src_ref=src.at[dest // BATCHES * BATCHES + b, :, half(lax.rem(dest, BATCHES))],
            dst_ref=held.at[block(me), half(core)],
            send_sem=f_send.at[b, place(dest)],
            recv_sem=f_recv.at[core, place(dest)],
            device_id=(dest, 2 * x + b),
            device_id_type=MESH,
        )

    def forward_in(other, i):
        return pltpu.make_async_remote_copy(
            src_ref=src.at[0, :, half(0)],
            dst_ref=held.at[block(0), half(0)],
            send_sem=f_send.at[other, i],
            recv_sem=f_recv.at[other, i],
            device_id=(me, 2 * x + 1 - core),
            device_id_type=MESH,
        )

    def backward(b, dest):
        return pltpu.make_async_remote_copy(
            src_ref=upd.at[block(dest), half(b)],
            dst_ref=ret.at[mine, :, half(seat)],
            send_sem=b_send.at[b, place(dest)],
            recv_sem=b_recv.at[core, place(dest)],
            device_id=(dest, 2 * x + b),
            device_id_type=MESH,
        )

    def backward_in(other, i):
        return pltpu.make_async_remote_copy(
            src_ref=upd.at[block(0), half(0)],
            dst_ref=ret.at[0, :, half(0)],
            send_sem=b_send.at[other, i],
            recv_sem=b_recv.at[other, i],
            device_id=(me, 2 * x + 1 - core),
            device_id_type=MESH,
        )

    keep_forward = pltpu.make_async_copy(
        src.at[mine, :, half(seat)], held.at[block(me), half(core)], local.at[0]
    )
    keep_backward = pltpu.make_async_copy(
        upd.at[block(me), half(core)], ret.at[mine, :, half(seat)], local.at[1]
    )

    def each(low, high, do):
        def body(i, c):
            do(i)
            return c

        lax.fori_loop(low, high, body, 0)

    my_slice = pl.ds(pl.multiple_of(rank * SLICE, 16), SLICE)

    def scatter(j):
        device, other = mate(j)
        return pltpu.make_async_remote_copy(
            src_ref=packed.at[pl.ds(pl.multiple_of(other * SLICE, 16), SLICE)],
            dst_ref=slots.at[j],
            send_sem=r_send.at[j],
            recv_sem=r_recv.at[j],
            device_id=device,
            device_id_type=MESH,
        )

    def gather(j):
        device, _ = mate(j)
        return pltpu.make_async_remote_copy(
            src_ref=own,
            dst_ref=full.at[my_slice],
            send_sem=g_send.at[j],
            recv_sem=g_recv.at[j],
            device_id=device,
            device_id_type=MESH,
        )

    for b in range(2):
        each(YS, YS + OUT - 1, lambda i: forward(b, partner(i)).start())
        pl.when(core != b)(lambda: forward(b, me).start())
    keep_forward.start()

    def others(do):
        for other in range(2):
            each(1, OUT, lambda i: do(other, i))
            pl.when(core != other)(lambda: do(other, 0))

    keep_forward.wait()
    others(lambda other, i: forward_in(other, i).wait_recv())
    top = dot_t(held[0:256, :], held[...]).astype(BF16)
    low = dot_t(held[256:512, :], held[256:512, :]).astype(BF16)
    for n, (i, j) in enumerate(PIECES):
        rows, cols = (128 * i, 128 * j) if i < 2 else (128 * i - 256, 128 * j - 256)
        packed[128 * n : 128 * n + 128, :] = (top if i < 2 else low)[rows : rows + 128, cols : cols + 128]
    each(1, GROUP, lambda j: scatter(j).start())
    each(1, GROUP, lambda j: scatter(j).wait_recv())
    total = packed[my_slice, :].astype(F32)
    for j in range(1, GROUP):
        total = total + slots[j].astype(F32)
    own[...] = total
    full[my_slice, :] = total
    each(1, GROUP, lambda j: gather(j).start())
    each(1, GROUP, lambda j: gather(j).wait_recv())

    R, Q, M, Y = (rh, rl), (qh, ql), (mh, ml), (yh, yl)

    def eye(x):
        rows = lax.broadcasted_iota(jnp.int32, x.shape, 0)
        cols = lax.broadcasted_iota(jnp.int32, x.shape, 1)
        return rows == cols

    def poly():
        m = COEF_C * product(R, R) + COEF_B * (rh[...].astype(F32) + rl[...].astype(F32))
        put(M, m + jnp.where(eye(m), COEF_A, 0.0))

    def advance():
        put(Y, product(M, R))
        put(R, product(Y, M))

    trace = jnp.zeros((), F32)
    for n, (i, j) in enumerate(PIECES):
        if i == j:
            part = full[128 * n : 128 * n + 128, :]
            trace = trace + jnp.sum(jnp.where(eye(part), part, 0.0))
    scale2 = trace + EPSILON
    inverse = 1.0 / jnp.full((1, 128), scale2, F32)
    for n, (i, j) in enumerate(PIECES):
        part = full[128 * n : 128 * n + 128, :] * inverse
        high, low = split(part)
        rows, cols = slice(128 * i, 128 * i + 128), slice(128 * j, 128 * j + 128)
        rh[rows, cols] = high
        rl[rows, cols] = low
        if i != j:
            high, low = split(part.T)
            rh[cols, rows] = high
            rl[cols, rows] = low
    def first_factor():
        qh[...] = mh[...]
        ql[...] = ml[...]

    def sweep(i):
        poly()
        pl.when(i == 0)(first_factor)
        pl.when(i > 0)(lambda: put(Q, product(Q, M)))
        advance()

    each(0, ITERS - 1, sweep)
    poly()
    factor[...] = (product(Q, M) * (1.0 / jnp.sqrt(jnp.full((1, ROWS), scale2, F32)))).astype(BF16)

    def strip(c):
        chip = lax.rem(z // 2 + c, ZS // 2)
        rows = pl.ds(pl.multiple_of(chip * 128, 128), 128)
        upd[rows, :] = (0.2 * math.sqrt(COLS) * dot(factor[rows, :], held[...])).astype(BF16)

        def send(i):
            dest = chip * 8 + i // 2
            b = lax.rem(i, 2)
            pl.when(jnp.logical_or(dest != me, b != core))(lambda: backward(b, dest).start())

        each(0, 16, send)

    each(0, ZS // 2, strip)
    keep_backward.start()
    keep_moment.wait()
    each(1, GROUP, lambda j: scatter(j).wait_send())
    each(1, GROUP, lambda j: gather(j).wait_send())
    others(lambda other, i: forward_in(other, i).wait_send())
    keep_backward.wait()
    others(lambda other, i: backward_in(other, i).wait_send())
    others(lambda other, i: backward_in(other, i).wait_recv())


def exchange(gradient, momentum):
    matrix = pltpu.VMEM((ROWS, ROWS), BF16)
    staged = pltpu.VMEM(gradient.shape, BF16)
    dma = pltpu.SemaphoreType.DMA
    return pl.pallas_call(
        kernel,
        out_shape=(
            jax.ShapeDtypeStruct((OUT, BLOCK, WIDTH), BF16),
            jax.ShapeDtypeStruct(momentum.shape, BF16),
        ),
        in_specs=[pl.BlockSpec(memory_space=pltpu.HBM)] * 2,
        out_specs=[pl.BlockSpec(memory_space=pl.ANY)] * 2,
        scratch_shapes=[
            pltpu.VMEM((OUT, BLOCK, WIDTH), BF16),
            pltpu.VMEM((ROWS, WIDTH), BF16),
            pltpu.VMEM((ROWS, WIDTH), BF16),
            pltpu.VMEM((TALL, 128), BF16),
            pltpu.VMEM((GROUP, SLICE, 128), BF16),
            pltpu.VMEM((SLICE, 128), F32),
            pltpu.VMEM((TALL, 128), F32),
            *[matrix] * 9,
            staged, staged, staged,
            dma((2, OUT)), dma((2, OUT)), dma((2, OUT)), dma((2, OUT)),
            dma((GROUP,)), dma((GROUP,)), dma((GROUP,)), dma((GROUP,)),
            dma((2,)), dma((2,)), dma,
        ],
        compiler_params=pltpu.CompilerParams(
            collective_id=0, has_side_effects=True, vmem_limit_bytes=VMEM_LIMIT
        ),
        name="muon",
    )(gradient, momentum)


def on_device(weight, gradient, momentum):
    returned, momentum_next = exchange(gradient, momentum)
    weight_next = 0.9 * weight - 0.5 * returned[:, :, : weight.shape[2]].astype(F32)
    return (weight_next, momentum_next)


def solution(mesh):
    spec = P(None, "out", "inp")
    return jax.shard_map(
        on_device, mesh=mesh, in_specs=(spec, spec, spec), out_specs=(spec, spec), check_vma=False
    )
```

```python
import functools
import math

import jax
import jax.numpy as jnp
from jax import lax
from jax.experimental import pallas as pl
from jax.experimental.pallas import tpu as pltpu
from jax.sharding import PartitionSpec as P

ITERS = 5
COLS = 13824
BETA = 0.95
EPSILON = 1e-06
COEF_A = 3.4445
COEF_B = -4.775
COEF_C = 2.0315

MESH = pl.DeviceIdType.MESH
BF16 = jnp.bfloat16
F32 = jnp.float32

ZS, YS, INP = 8, 4, 8
OUT = ZS * YS
XS = INP // 2
LOCAL = 2
BATCHES = 2 * LOCAL
ROWS = 512
BLOCK = 16
WIDTH = 1792
WIDE, SLIM = 512, 384
PIECES_OF = [(0, WIDE), (512, WIDE), (1024, SLIM), (1408, SLIM)]
GROUP = XS * YS
PIECES = [(i, j) for i in range(4) for j in range(i, 4)]
TALL = 128 * len(PIECES)
SLICE = TALL // GROUP
VMEM_LIMIT = 50 * 2**20


def dot(a, b):
    return lax.dot_general(a, b, (((1,), (0,)), ((), ())), preferred_element_type=F32)


def dot_t(a, b):
    return lax.dot_general(a, b, (((1,), (1,)), ((), ())), preferred_element_type=F32)


def split(x):
    high = x.astype(BF16)
    return high, (x - high.astype(F32)).astype(BF16)


def product(a, b):
    return dot(a[0][...], b[0][...]) + dot(a[0][...], b[1][...]) + dot(a[1][...], b[0][...])


def put(pair, x):
    high, low = split(x)
    pair[0][...] = high
    pair[1][...] = low


def kernel(
    grad, mom, ret, mom_next, src, held, upd, packed, slots, own, full, factor,
    rh, rl, qh, ql, mh, ml, yh, yl, grad_in, mom_in, mom_out,
    f_send, f_recv, b_send, b_recv, r_send, r_recv, g_send, g_recv, local, load, store,
):
    me = lax.axis_index("out")
    inp = lax.axis_index("inp")
    z, y = me // YS, lax.rem(me, YS)
    x, core = inp // 2, lax.rem(inp, 2)
    rank = y * XS + x
    width = grad.shape[2]

    def mine(l):
        return z * BATCHES + 2 * l + core

    loads = [
        pltpu.make_async_copy(grad, grad_in, load.at[0]),
        pltpu.make_async_copy(mom, mom_in, load.at[1]),
    ]
    for copy in loads:
        copy.start()

    def each(low, high, do):
        def body(i, c):
            do(i)
            return c

        lax.fori_loop(low, high, body, 0)

    def by_width(do):
        pl.when(y < 2)(lambda: do(WIDE, pl.multiple_of(y * WIDE, 128)))
        pl.when(y >= 2)(lambda: do(SLIM, pl.multiple_of(2 * WIDE + (y - 2) * SLIM, 128)))

    def clear():
        for l in range(LOCAL):
            for c in range(2):
                held[l, :, c * WIDE + SLIM : c * WIDE + WIDE] = jnp.zeros((ROWS, WIDE - SLIM), BF16)

    pl.when(y >= 2)(clear)

    def mate(j):
        other = lax.rem(rank + j, GROUP)
        return (z * YS + other // XS, 2 * lax.rem(other, XS) + core), other

    barrier = pltpu.get_barrier_semaphore()

    def greet(i):
        dest = lax.rem(me + i, OUT)
        for other in range(2):
            pl.semaphore_signal(barrier, inc=1, device_id=(dest, 2 * x + other), device_id_type=MESH)

    def greet_mate(j):
        pl.semaphore_signal(barrier, inc=1, device_id=mate(j)[0], device_id_type=MESH)

    each(1, OUT, greet)
    each(1, GROUP, greet_mate)
    pl.semaphore_signal(barrier, inc=1, device_id=(me, 2 * x + 1 - core), device_id_type=MESH)
    for copy in loads:
        copy.wait()

    def elementwise(k):
        g = grad_in[k].astype(F32)
        moment = BETA * mom_in[k].astype(F32) + g
        mom_out[k] = moment.astype(BF16)
        src[k, :, 0:width] = (g + BETA * moment).astype(BF16)
        src[k, :, width:WIDTH] = jnp.zeros((BLOCK, WIDTH - width), BF16)

    each(0, OUT, elementwise)
    keep_moment = pltpu.make_async_copy(mom_out, mom_next, store)
    keep_moment.start()
    pl.semaphore_wait(barrier, 2 * (OUT - 1) + GROUP - 1 + 1)

    def block(dest):
        return pl.ds(pl.multiple_of(dest * BLOCK, BLOCK), BLOCK)

    def part(which, wide):
        return pl.ds(pl.multiple_of(which * WIDE, 128), wide)

    def place(dest):
        return lax.rem(dest // YS - z + ZS, ZS) * YS + lax.rem(lax.rem(dest, YS) - y + YS, YS)

    def forward(b, chip, yd):
        dest = chip * YS + yd
        offset, wide = PIECES_OF[yd]
        return pltpu.make_async_remote_copy(
            src_ref=src.at[chip * BATCHES + b, :, offset : offset + wide],
            dst_ref=held.at[b // 2, block(me), part(core, wide)],
            send_sem=f_send.at[b, place(dest)],
            recv_sem=f_recv.at[b // 2 * 2 + core, place(dest)],
            device_id=(dest, 2 * x + b % 2),
            device_id_type=MESH,
        )

    def forward_in(l, other, i, wide):
        return pltpu.make_async_remote_copy(
            src_ref=src.at[0, :, 0:wide],
            dst_ref=held.at[l, block(0), part(0, wide)],
            send_sem=f_send.at[2 * l + other, i],
            recv_sem=f_recv.at[2 * l + other, i],
            device_id=(me, 2 * x + 1 - core),
            device_id_type=MESH,
        )

    def backward(l, b, dest, wide, offset):
        return pltpu.make_async_remote_copy(
            src_ref=upd.at[l, block(dest), part(b, wide)],
            dst_ref=ret.at[mine(l), :, pl.ds(offset, wide)],
            send_sem=b_send.at[2 * l + b, place(dest)],
            recv_sem=b_recv.at[2 * l + core, place(dest)],
            device_id=(dest, 2 * x + b),
            device_id_type=MESH,
        )

    def backward_in(l, other, i, wide):
        return pltpu.make_async_remote_copy(
            src_ref=upd.at[l, block(0), part(0, wide)],
            dst_ref=ret.at[0, :, 0:wide],
            send_sem=b_send.at[2 * l + other, i],
            recv_sem=b_recv.at[2 * l + other, i],
            device_id=(me, 2 * x + 1 - core),
            device_id_type=MESH,
        )

    def keep_forward(l, wide, offset):
        return pltpu.make_async_copy(
            src.at[mine(l), :, pl.ds(offset, wide)], held.at[l, block(me), part(core, wide)], local.at[0, l]
        )

    def keep_backward(l, wide, offset):
        return pltpu.make_async_copy(
            upd.at[l, block(me), part(core, wide)], ret.at[mine(l), :, pl.ds(offset, wide)], local.at[1, l]
        )

    my_slice = pl.ds(pl.multiple_of(rank * SLICE, 16), SLICE)

    def scatter(l, j):
        device, other = mate(j)
        return pltpu.make_async_remote_copy(
            src_ref=packed.at[l, pl.ds(pl.multiple_of(other * SLICE, 16), SLICE)],
            dst_ref=slots.at[l, j],
            send_sem=r_send.at[l, j],
            recv_sem=r_recv.at[l, j],
            device_id=device,
            device_id_type=MESH,
        )

    def gather(l, j):
        device, _ = mate(j)
        return pltpu.make_async_remote_copy(
            src_ref=own.at[l],
            dst_ref=full.at[l, my_slice],
            send_sem=g_send.at[l, j],
            recv_sem=g_recv.at[l, j],
            device_id=device,
            device_id_type=MESH,
        )

    def all_forward(b, do):
        def body(i):
            t = lax.rem(i, ZS)
            step = jnp.where(lax.rem(t, 2) == 1, (t + 1) // 2, ZS - t // 2)
            chip = lax.rem(z + step, ZS)
            for yd in range(YS):
                away = jnp.logical_or(chip * YS + yd != me, core != b % 2)
                pl.when(away)(lambda: do(forward(b, chip, yd)))

        each(1, ZS + 1, body)

    def others(do):
        for other in range(2):
            each(1, OUT, lambda i: do(other, i))
            pl.when(core != other)(lambda: do(other, 0))

    for b in range(BATCHES):
        all_forward(b, lambda copy: copy.start())
    for l in range(LOCAL):
        by_width(lambda wide, offset: keep_forward(l, wide, offset).start())

    def gram(l):
        by_width(lambda wide, offset: keep_forward(l, wide, offset).wait())
        by_width(lambda wide, offset: others(lambda other, i: forward_in(l, other, i, wide).wait_recv()))
        top = dot_t(held[l, 0:256, :], held[l]).astype(BF16)
        low = dot_t(held[l, 256:512, :], held[l, 256:512, :]).astype(BF16)
        for n, (i, j) in enumerate(PIECES):
            rows, cols = (128 * i, 128 * j) if i < 2 else (128 * i - 256, 128 * j - 256)
            packed[l, 128 * n : 128 * n + 128, :] = (top if i < 2 else low)[rows : rows + 128, cols : cols + 128]
        each(1, GROUP, lambda j: scatter(l, j).start())

    def reduce(l):
        each(1, GROUP, lambda j: scatter(l, j).wait_recv())
        total = packed[l, my_slice, :].astype(F32)
        for j in range(1, GROUP):
            total = total + slots[l, j].astype(F32)
        own[l] = total
        full[l, my_slice, :] = total
        each(1, GROUP, lambda j: gather(l, j).start())

    R, Q, M, Y = (rh, rl), (qh, ql), (mh, ml), (yh, yl)

    def eye(x):
        rows = lax.broadcasted_iota(jnp.int32, x.shape, 0)
        cols = lax.broadcasted_iota(jnp.int32, x.shape, 1)
        return rows == cols

    def poly():
        m = COEF_C * product(R, R) + COEF_B * (rh[...].astype(F32) + rl[...].astype(F32))
        put(M, m + jnp.where(eye(m), COEF_A, 0.0))

    def advance():
        put(Y, product(M, R))
        put(R, product(Y, M))

    def first_factor():
        qh[...] = mh[...]
        ql[...] = ml[...]

    def turn(l):
        each(1, GROUP, lambda j: gather(l, j).wait_recv())
        trace = jnp.zeros((), F32)
        for n, (i, j) in enumerate(PIECES):
            if i == j:
                piece = full[l, 128 * n : 128 * n + 128, :]
                trace = trace + jnp.sum(jnp.where(eye(piece), piece, 0.0))
        scale2 = trace + EPSILON
        inverse = 1.0 / jnp.full((1, 128), scale2, F32)
        for n, (i, j) in enumerate(PIECES):
            piece = full[l, 128 * n : 128 * n + 128, :] * inverse
            high, low = split(piece)
            rows, cols = slice(128 * i, 128 * i + 128), slice(128 * j, 128 * j + 128)
            rh[rows, cols] = high
            rl[rows, cols] = low
            if i != j:
                high, low = split(piece.T)
                rh[cols, rows] = high
                rl[cols, rows] = low

        def sweep(i):
            poly()
            pl.when(i == 0)(first_factor)
            pl.when(i > 0)(lambda: put(Q, product(Q, M)))
            advance()
            pl.when(jnp.logical_and(l == 0, i == 2))(lambda: gram(1))

        each(0, ITERS - 1, sweep)
        poly()
        factor[...] = (product(Q, M) * (1.0 / jnp.sqrt(jnp.full((1, ROWS), scale2, F32)))).astype(BF16)
        pl.when(l == 0)(lambda: reduce(1))

        def strip(c):
            chips = lax.rem(z // 2 + c, ZS // 2)
            rows = pl.ds(pl.multiple_of(chips * 128, 128), 128)
            upd[l, rows, :] = (0.2 * math.sqrt(COLS) * dot(factor[rows, :], held[l])).astype(BF16)

            def send(wide, offset):
                def one(i):
                    dest = chips * 8 + i // 2
                    b = lax.rem(i, 2)
                    away = jnp.logical_or(dest != me, b != core)
                    pl.when(away)(lambda: backward(l, b, dest, wide, offset).start())

                each(0, 16, one)

            by_width(send)

        each(0, ZS // 2, strip)
        by_width(lambda wide, offset: keep_backward(l, wide, offset).start())

    gram(0)
    reduce(0)
    each(0, LOCAL, turn)
    keep_moment.wait()
    for b in range(BATCHES):
        all_forward(b, lambda copy: copy.wait_send())
    for l in range(LOCAL):
        each(1, GROUP, lambda j: scatter(l, j).wait_send())
        each(1, GROUP, lambda j: gather(l, j).wait_send())
        by_width(lambda wide, offset: keep_backward(l, wide, offset).wait())
        by_width(lambda wide, offset: others(lambda other, i: backward_in(l, other, i, wide).wait_send()))
    for l in range(LOCAL):
        for other in range(2):
            for ys in range(YS):
                wide = PIECES_OF[ys][1]
                behind = lax.rem(y - ys + YS, YS)

                def arrive(step):
                    away = jnp.logical_or(step * YS + behind != 0, core != other)
                    pl.when(away)(lambda: backward_in(l, other, step * YS + behind, wide).wait_recv())

                each(0, ZS, arrive)


def exchange(gradient, momentum):
    matrix = pltpu.VMEM((ROWS, ROWS), BF16)
    staged = pltpu.VMEM(gradient.shape, BF16)
    dma = pltpu.SemaphoreType.DMA
    return pl.pallas_call(
        kernel,
        out_shape=(
            jax.ShapeDtypeStruct((OUT, BLOCK, WIDTH), BF16),
            jax.ShapeDtypeStruct(momentum.shape, BF16),
        ),
        in_specs=[pl.BlockSpec(memory_space=pltpu.HBM)] * 2,
        out_specs=[pl.BlockSpec(memory_space=pl.ANY)] * 2,
        scratch_shapes=[
            pltpu.VMEM((OUT, BLOCK, WIDTH), BF16),
            pltpu.VMEM((LOCAL, ROWS, 2 * WIDE), BF16),
            pltpu.VMEM((LOCAL, ROWS, 2 * WIDE), BF16),
            pltpu.VMEM((LOCAL, TALL, 128), BF16),
            pltpu.VMEM((LOCAL, GROUP, SLICE, 128), BF16),
            pltpu.VMEM((LOCAL, SLICE, 128), F32),
            pltpu.VMEM((LOCAL, TALL, 128), F32),
            *[matrix] * 9,
            staged, staged, staged,
            dma((BATCHES, OUT)), dma((BATCHES, OUT)), dma((BATCHES, OUT)), dma((BATCHES, OUT)),
            dma((LOCAL, GROUP)), dma((LOCAL, GROUP)), dma((LOCAL, GROUP)), dma((LOCAL, GROUP)),
            dma((2, LOCAL)), dma((2,)), dma,
        ],
        compiler_params=pltpu.CompilerParams(
            collective_id=0, has_side_effects=True, vmem_limit_bytes=VMEM_LIMIT
        ),
        name="muon",
    )(gradient, momentum)


def on_device(weight, gradient, momentum):
    returned, momentum_next = exchange(gradient, momentum)
    weight_next = 0.9 * weight - 0.5 * returned[:, :, : weight.shape[2]].astype(F32)
    return (weight_next, momentum_next)


def solution(mesh):
    spec = P(None, "out", "inp")
    return jax.shard_map(
        on_device, mesh=mesh, in_specs=(spec, spec, spec), out_specs=(spec, spec), check_vma=False
    )
```

```python
import functools
import math

import jax
import jax.numpy as jnp
from jax import lax
from jax.experimental import pallas as pl
from jax.experimental.pallas import tpu as pltpu
from jax.sharding import PartitionSpec as P

ITERS = 5
COLS = 13824
BETA = 0.95
EPSILON = 1e-06
COEF_A = 3.4445
COEF_B = -4.775
COEF_C = 2.0315

MESH = pl.DeviceIdType.MESH
BF16 = jnp.bfloat16
F32 = jnp.float32

ZS, YS, INP = 8, 4, 8
OUT = ZS * YS
BATCHES = 2
ROWS = 512
BLOCK = 16
WIDTH = 1792
HALF = WIDTH // BATCHES
GROUP = INP // 2 * BATCHES
PIECES = [(i, j) for i in range(4) for j in range(i, 4)]
TALL = 128 * len(PIECES)
SLICE = TALL // GROUP
VMEM_LIMIT = 50 * 2**20


def dot(a, b):
    return lax.dot_general(a, b, (((1,), (0,)), ((), ())), preferred_element_type=F32)


def dot_t(a, b):
    return lax.dot_general(a, b, (((1,), (1,)), ((), ())), preferred_element_type=F32)


def split(x):
    high = x.astype(BF16)
    return high, (x - high.astype(F32)).astype(BF16)


def product(a, b):
    return dot(a[0][...], b[0][...]) + dot(a[0][...], b[1][...]) + dot(a[1][...], b[0][...])


def put(pair, x):
    high, low = split(x)
    pair[0][...] = high
    pair[1][...] = low


def kernel(
    grad, mom, ret, mom_next, src, held, upd, packed, slots, own, full, factor,
    rh, rl, qh, ql, mh, ml, yh, yl, grad_in, mom_in, mom_out,
    f_send, f_recv, b_send, b_recv, r_send, r_recv, g_send, g_recv, local, load, store,
):
    me = lax.axis_index("out")
    inp = lax.axis_index("inp")
    z, y = me // YS, lax.rem(me, YS)
    team, seat = me // BATCHES, lax.rem(me, BATCHES)
    x, core = inp // 2, lax.rem(inp, 2)
    rank = seat * (INP // 2) + x
    mine = team * BATCHES + core
    width = grad.shape[2]

    loads = [
        pltpu.make_async_copy(grad, grad_in, load.at[0]),
        pltpu.make_async_copy(mom, mom_in, load.at[1]),
    ]
    for copy in loads:
        copy.start()

    def partner(i):
        at = lax.rem(i, OUT) + i // OUT
        t = at // YS
        step = jnp.where(lax.rem(t, 2) == 1, (t + 1) // 2, ZS - t // 2)
        return lax.rem(z + step, ZS) * YS + lax.rem(y + lax.rem(at, YS), YS)

    def mate(j):
        other = lax.rem(rank + j, GROUP)
        return (team * BATCHES + other // (INP // 2), 2 * lax.rem(other, INP // 2) + core), other

    barrier = pltpu.get_barrier_semaphore()

    def greet(i, c):
        dest = lax.rem(me + i, OUT)
        for other in range(2):
            pl.semaphore_signal(barrier, inc=1, device_id=(dest, 2 * x + other), device_id_type=MESH)
        return c

    def greet_mate(j, c):
        pl.semaphore_signal(barrier, inc=1, device_id=mate(j)[0], device_id_type=MESH)
        return c

    lax.fori_loop(1, OUT, greet, 0)
    lax.fori_loop(1, GROUP, greet_mate, 0)
    pl.semaphore_signal(barrier, inc=1, device_id=(me, 2 * x + 1 - core), device_id_type=MESH)

    for copy in loads:
        copy.wait()

    def elementwise(k, c):
        g = grad_in[k].astype(F32)
        moment = BETA * mom_in[k].astype(F32) + g
        mom_out[k] = moment.astype(BF16)
        src[k, :, 0:width] = (g + BETA * moment).astype(BF16)
        src[k, :, width:WIDTH] = jnp.zeros((BLOCK, WIDTH - width), BF16)
        return c

    lax.fori_loop(0, OUT, elementwise, 0)
    keep_moment = pltpu.make_async_copy(mom_out, mom_next, store)
    keep_moment.start()
    pl.semaphore_wait(barrier, 2 * (OUT - 1) + GROUP - 1 + 1)

    def block(dest):
        return pl.ds(pl.multiple_of(dest * BLOCK, BLOCK), BLOCK)

    def half(which):
        return pl.ds(pl.multiple_of(which * HALF, 128), HALF)

    def place(dest):
        return lax.rem(dest // YS - z + ZS, ZS) * YS + lax.rem(lax.rem(dest, YS) - y + YS, YS)

    def forward(b, dest):
        return pltpu.make_async_remote_copy(
            src_ref=src.at[dest // BATCHES * BATCHES + b, :, half(lax.rem(dest, BATCHES))],
            dst_ref=held.at[block(me), half(core)],
            send_sem=f_send.at[b, place(dest)],
            recv_sem=f_recv.at[core, place(dest)],
            device_id=(dest, 2 * x + b),
            device_id_type=MESH,
        )

    def forward_in(other, i):
        return pltpu.make_async_remote_copy(
            src_ref=src.at[0, :, half(0)],
            dst_ref=held.at[block(0), half(0)],
            send_sem=f_send.at[other, i],
            recv_sem=f_recv.at[other, i],
            device_id=(me, 2 * x + 1 - core),
            device_id_type=MESH,
        )

    def backward(b, dest):
        return pltpu.make_async_remote_copy(
            src_ref=upd.at[block(dest), half(b)],
            dst_ref=ret.at[mine, :, half(seat)],
            send_sem=b_send.at[b, place(dest)],
            recv_sem=b_recv.at[core, place(dest)],
            device_id=(dest, 2 * x + b),
            device_id_type=MESH,
        )

    def backward_in(other, i):
        return pltpu.make_async_remote_copy(
            src_ref=upd.at[block(0), half(0)],
            dst_ref=ret.at[0, :, half(0)],
            send_sem=b_send.at[other, i],
            recv_sem=b_recv.at[other, i],
            device_id=(me, 2 * x + 1 - core),
            device_id_type=MESH,
        )

    keep_forward = pltpu.make_async_copy(
        src.at[mine, :, half(seat)], held.at[block(me), half(core)], local.at[0]
    )
    keep_backward = pltpu.make_async_copy(
        upd.at[block(me), half(core)], ret.at[mine, :, half(seat)], local.at[1]
    )

    def each(low, high, do):
        def body(i, c):
            do(i)
            return c

        lax.fori_loop(low, high, body, 0)

    my_slice = pl.ds(pl.multiple_of(rank * SLICE, 16), SLICE)

    def scatter(j):
        device, other = mate(j)
        return pltpu.make_async_remote_copy(
            src_ref=packed.at[pl.ds(pl.multiple_of(other * SLICE, 16), SLICE)],
            dst_ref=slots.at[j],
            send_sem=r_send.at[j],
            recv_sem=r_recv.at[j],
            device_id=device,
            device_id_type=MESH,
        )

    def gather(j):
        device, _ = mate(j)
        return pltpu.make_async_remote_copy(
            src_ref=own,
            dst_ref=full.at[my_slice],
            send_sem=g_send.at[j],
            recv_sem=g_recv.at[j],
            device_id=device,
            device_id_type=MESH,
        )

    def send_on(low, high):
        each(low, high, lambda i: forward(1, partner(i)).start())

    each(YS, YS + OUT - 1, lambda i: forward(0, partner(i)).start())
    pl.when(core != 0)(lambda: forward(0, me).start())
    send_on(YS, 4 * YS)
    pl.when(core != 1)(lambda: forward(1, me).start())
    pl.when(core != 0)(lambda: send_on(4 * YS, YS + OUT - 1))
    keep_forward.start()

    def others(do):
        for other in range(2):
            each(1, OUT, lambda i: do(other, i))
            pl.when(core != other)(lambda: do(other, 0))

    keep_forward.wait()
    others(lambda other, i: forward_in(other, i).wait_recv())
    top = dot_t(held[0:256, :], held[...]).astype(BF16)
    low = dot_t(held[256:512, :], held[256:512, :]).astype(BF16)
    for n, (i, j) in enumerate(PIECES):
        rows, cols = (128 * i, 128 * j) if i < 2 else (128 * i - 256, 128 * j - 256)
        packed[128 * n : 128 * n + 128, :] = (top if i < 2 else low)[rows : rows + 128, cols : cols + 128]
    each(1, GROUP, lambda j: scatter(j).start())
    pl.when(core == 0)(lambda: send_on(4 * YS, 6 * YS))
    each(1, GROUP, lambda j: scatter(j).wait_recv())
    total = packed[my_slice, :].astype(F32)
    for j in range(1, GROUP):
        total = total + slots[j].astype(F32)
    own[...] = total
    full[my_slice, :] = total
    each(1, GROUP, lambda j: gather(j).start())
    pl.when(core == 0)(lambda: send_on(6 * YS, YS + OUT - 1))
    each(1, GROUP, lambda j: gather(j).wait_recv())

    R, Q, M, Y = (rh, rl), (qh, ql), (mh, ml), (yh, yl)

    def eye(x):
        rows = lax.broadcasted_iota(jnp.int32, x.shape, 0)
        cols = lax.broadcasted_iota(jnp.int32, x.shape, 1)
        return rows == cols

    def poly():
        m = COEF_C * product(R, R) + COEF_B * (rh[...].astype(F32) + rl[...].astype(F32))
        put(M, m + jnp.where(eye(m), COEF_A, 0.0))

    def advance():
        put(Y, product(M, R))
        put(R, product(Y, M))

    trace = jnp.zeros((), F32)
    for n, (i, j) in enumerate(PIECES):
        if i == j:
            part = full[128 * n : 128 * n + 128, :]
            trace = trace + jnp.sum(jnp.where(eye(part), part, 0.0))
    scale2 = trace + EPSILON
    inverse = 1.0 / jnp.full((1, 128), scale2, F32)
    for n, (i, j) in enumerate(PIECES):
        part = full[128 * n : 128 * n + 128, :] * inverse
        high, low = split(part)
        rows, cols = slice(128 * i, 128 * i + 128), slice(128 * j, 128 * j + 128)
        rh[rows, cols] = high
        rl[rows, cols] = low
        if i != j:
            high, low = split(part.T)
            rh[cols, rows] = high
            rl[cols, rows] = low
    def first_factor():
        qh[...] = mh[...]
        ql[...] = ml[...]

    def sweep(i):
        poly()
        pl.when(i == 0)(first_factor)
        pl.when(i > 0)(lambda: put(Q, product(Q, M)))
        advance()

    each(0, ITERS - 1, sweep)
    poly()
    factor[...] = (product(Q, M) * (1.0 / jnp.sqrt(jnp.full((1, ROWS), scale2, F32)))).astype(BF16)

    def strip(c):
        chip = lax.rem(z // 2 + c, ZS // 2)
        rows = pl.ds(pl.multiple_of(chip * 128, 128), 128)
        upd[rows, :] = (0.2 * math.sqrt(COLS) * dot(factor[rows, :], held[...])).astype(BF16)

        def send(i):
            dest = chip * 8 + i // 2
            b = lax.rem(i, 2)
            pl.when(jnp.logical_or(dest != me, b != core))(lambda: backward(b, dest).start())

        each(0, 16, send)

    each(0, ZS // 2, strip)
    keep_backward.start()
    keep_moment.wait()
    each(1, GROUP, lambda j: scatter(j).wait_send())
    each(1, GROUP, lambda j: gather(j).wait_send())
    others(lambda other, i: forward_in(other, i).wait_send())
    keep_backward.wait()
    others(lambda other, i: backward_in(other, i).wait_send())
    others(lambda other, i: backward_in(other, i).wait_recv())


def exchange(gradient, momentum):
    matrix = pltpu.VMEM((ROWS, ROWS), BF16)
    staged = pltpu.VMEM(gradient.shape, BF16)
    dma = pltpu.SemaphoreType.DMA
    return pl.pallas_call(
        kernel,
        out_shape=(
            jax.ShapeDtypeStruct((OUT, BLOCK, WIDTH), BF16),
            jax.ShapeDtypeStruct(momentum.shape, BF16),
        ),
        in_specs=[pl.BlockSpec(memory_space=pltpu.HBM)] * 2,
        out_specs=[pl.BlockSpec(memory_space=pl.ANY)] * 2,
        scratch_shapes=[
            pltpu.VMEM((OUT, BLOCK, WIDTH), BF16),
            pltpu.VMEM((ROWS, WIDTH), BF16),
            pltpu.VMEM((ROWS, WIDTH), BF16),
            pltpu.VMEM((TALL, 128), BF16),
            pltpu.VMEM((GROUP, SLICE, 128), BF16),
            pltpu.VMEM((SLICE, 128), F32),
            pltpu.VMEM((TALL, 128), F32),
            *[matrix] * 9,
            staged, staged, staged,
            dma((2, OUT)), dma((2, OUT)), dma((2, OUT)), dma((2, OUT)),
            dma((GROUP,)), dma((GROUP,)), dma((GROUP,)), dma((GROUP,)),
            dma((2,)), dma((2,)), dma,
        ],
        compiler_params=pltpu.CompilerParams(
            collective_id=0, has_side_effects=True, vmem_limit_bytes=VMEM_LIMIT
        ),
        name="muon",
    )(gradient, momentum)


def on_device(weight, gradient, momentum):
    returned, momentum_next = exchange(gradient, momentum)
    weight_next = 0.9 * weight - 0.5 * returned[:, :, : weight.shape[2]].astype(F32)
    return (weight_next, momentum_next)


def solution(mesh):
    spec = P(None, "out", "inp")
    return jax.shard_map(
        on_device, mesh=mesh, in_specs=(spec, spec, spec), out_specs=(spec, spec), check_vma=False
    )
```

```python
import functools
import math

import jax
import jax.numpy as jnp
from jax import lax
from jax.experimental import pallas as pl
from jax.experimental.pallas import tpu as pltpu
from jax.sharding import PartitionSpec as P

ITERS = 5
COLS = 13824
BETA = 0.95
EPSILON = 1e-06
COEF_A = 3.4445
COEF_B = -4.775
COEF_C = 2.0315

MESH = pl.DeviceIdType.MESH
BF16 = jnp.bfloat16
F32 = jnp.float32

ZS, YS, INP = 8, 4, 8
OUT = ZS * YS
BATCHES = 2
ROWS = 512
BLOCK = 16
WIDTH = 1792
HALF = WIDTH // BATCHES
XS = INP // 2
GROUP = XS * BATCHES
PIECES = [(i, j) for i in range(4) for j in range(i, 4)]
TALL = 128 * len(PIECES)
SLICE = TALL // GROUP
VMEM_LIMIT = 50 * 2**20


def dot(a, b):
    return lax.dot_general(a, b, (((1,), (0,)), ((), ())), preferred_element_type=F32)


def dot_t(a, b):
    return lax.dot_general(a, b, (((1,), (1,)), ((), ())), preferred_element_type=F32)


def split(x):
    high = x.astype(BF16)
    return high, (x - high.astype(F32)).astype(BF16)


def product(a, b):
    return dot(a[0][...], b[0][...]) + dot(a[0][...], b[1][...]) + dot(a[1][...], b[0][...])


def put(pair, x):
    high, low = split(x)
    pair[0][...] = high
    pair[1][...] = low


def kernel(
    grad, mom, ret, mom_next, src, held, upd, packed, slots, own, full, factor,
    rh, rl, qh, ql, mh, ml, yh, yl, grad_in, mom_in, mom_out,
    f_send, f_recv, b_send, b_recv, r_send, r_recv, g_send, g_recv, local, load, store,
):
    me = lax.axis_index("out")
    inp = lax.axis_index("inp")
    z, y = me // YS, lax.rem(me, YS)
    team, seat = me // BATCHES, lax.rem(me, BATCHES)
    x, core = inp // 2, lax.rem(inp, 2)
    rank = seat * (INP // 2) + x
    mine = team * BATCHES + core
    width = grad.shape[2]

    loads = [
        pltpu.make_async_copy(grad, grad_in, load.at[0]),
        pltpu.make_async_copy(mom, mom_in, load.at[1]),
    ]
    for copy in loads:
        copy.start()

    def partner(i):
        at = lax.rem(i, OUT) + i // OUT
        t = at // YS
        step = jnp.where(lax.rem(t, 2) == 1, (t + 1) // 2, ZS - t // 2)
        return lax.rem(z + step, ZS) * YS + lax.rem(y + lax.rem(at, YS), YS)

    def mate(j):
        other_seat = lax.rem(seat + j // XS, BATCHES)
        other_x = lax.rem(x + lax.rem(j, XS), XS)
        return (team * BATCHES + other_seat, 2 * other_x + core), other_seat * XS + other_x

    barrier = pltpu.get_barrier_semaphore()

    def greet(i, c):
        dest = lax.rem(me + i, OUT)
        for other in range(2):
            pl.semaphore_signal(barrier, inc=1, device_id=(dest, 2 * x + other), device_id_type=MESH)
        return c

    def greet_mate(j, c):
        pl.semaphore_signal(barrier, inc=1, device_id=mate(j)[0], device_id_type=MESH)
        return c

    lax.fori_loop(1, OUT, greet, 0)
    lax.fori_loop(1, GROUP, greet_mate, 0)
    pl.semaphore_signal(barrier, inc=1, device_id=(me, 2 * x + 1 - core), device_id_type=MESH)

    for copy in loads:
        copy.wait()

    def elementwise(k, c):
        g = grad_in[k].astype(F32)
        moment = BETA * mom_in[k].astype(F32) + g
        mom_out[k] = moment.astype(BF16)
        src[k, :, 0:width] = (g + BETA * moment).astype(BF16)
        src[k, :, width:WIDTH] = jnp.zeros((BLOCK, WIDTH - width), BF16)
        return c

    lax.fori_loop(0, OUT, elementwise, 0)
    keep_moment = pltpu.make_async_copy(mom_out, mom_next, store)
    keep_moment.start()
    pl.semaphore_wait(barrier, 2 * (OUT - 1) + GROUP - 1 + 1)

    def block(dest):
        return pl.ds(pl.multiple_of(dest * BLOCK, BLOCK), BLOCK)

    def half(which):
        return pl.ds(pl.multiple_of(which * HALF, 128), HALF)

    def place(dest):
        return lax.rem(dest // YS - z + ZS, ZS) * YS + lax.rem(lax.rem(dest, YS) - y + YS, YS)

    def forward(b, dest):
        return pltpu.make_async_remote_copy(
            src_ref=src.at[dest // BATCHES * BATCHES + b, :, half(lax.rem(dest, BATCHES))],
            dst_ref=held.at[block(me), half(core)],
            send_sem=f_send.at[b, place(dest)],
            recv_sem=f_recv.at[core, place(dest)],
            device_id=(dest, 2 * x + b),
            device_id_type=MESH,
        )

    def forward_in(other, i):
        return pltpu.make_async_remote_copy(
            src_ref=src.at[0, :, half(0)],
            dst_ref=held.at[block(0), half(0)],
            send_sem=f_send.at[other, i],
            recv_sem=f_recv.at[other, i],
            device_id=(me, 2 * x + 1 - core),
            device_id_type=MESH,
        )

    def backward(b, dest):
        return pltpu.make_async_remote_copy(
            src_ref=upd.at[block(dest), half(b)],
            dst_ref=ret.at[mine, :, half(seat)],
            send_sem=b_send.at[b, place(dest)],
            recv_sem=b_recv.at[core, place(dest)],
            device_id=(dest, 2 * x + b),
            device_id_type=MESH,
        )

    def backward_in(other, i):
        return pltpu.make_async_remote_copy(
            src_ref=upd.at[block(0), half(0)],
            dst_ref=ret.at[0, :, half(0)],
            send_sem=b_send.at[other, i],
            recv_sem=b_recv.at[other, i],
            device_id=(me, 2 * x + 1 - core),
            device_id_type=MESH,
        )

    keep_forward = pltpu.make_async_copy(
        src.at[mine, :, half(seat)], held.at[block(me), half(core)], local.at[0]
    )
    keep_backward = pltpu.make_async_copy(
        upd.at[block(me), half(core)], ret.at[mine, :, half(seat)], local.at[1]
    )

    def each(low, high, do):
        def body(i, c):
            do(i)
            return c

        lax.fori_loop(low, high, body, 0)

    my_slice = pl.ds(pl.multiple_of(rank * SLICE, 16), SLICE)

    def scatter(j):
        device, other = mate(j)
        return pltpu.make_async_remote_copy(
            src_ref=packed.at[pl.ds(pl.multiple_of(other * SLICE, 16), SLICE)],
            dst_ref=slots.at[j],
            send_sem=r_send.at[j],
            recv_sem=r_recv.at[j],
            device_id=device,
            device_id_type=MESH,
        )

    def gather(j):
        device, _ = mate(j)
        return pltpu.make_async_remote_copy(
            src_ref=own,
            dst_ref=full.at[my_slice],
            send_sem=g_send.at[j],
            recv_sem=g_recv.at[j],
            device_id=device,
            device_id_type=MESH,
        )

    for b in range(2):
        each(YS, YS + OUT - 1, lambda i: forward(b, partner(i)).start())
        pl.when(core != b)(lambda: forward(b, me).start())
    keep_forward.start()

    def others(do):
        for other in range(2):
            each(1, OUT, lambda i: do(other, i))
            pl.when(core != other)(lambda: do(other, 0))

    keep_forward.wait()
    others(lambda other, i: forward_in(other, i).wait_recv())
    top = dot_t(held[0:256, :], held[...]).astype(BF16)
    low = dot_t(held[256:512, :], held[256:512, :]).astype(BF16)
    for n, (i, j) in enumerate(PIECES):
        rows, cols = (128 * i, 128 * j) if i < 2 else (128 * i - 256, 128 * j - 256)
        packed[128 * n : 128 * n + 128, :] = (top if i < 2 else low)[rows : rows + 128, cols : cols + 128]
    each(XS, GROUP, lambda j: scatter(j).start())
    each(1, XS, lambda j: scatter(j).start())
    each(1, GROUP, lambda j: scatter(j).wait_recv())
    total = packed[my_slice, :].astype(F32)
    for j in range(1, GROUP):
        total = total + slots[j].astype(F32)
    own[...] = total
    full[my_slice, :] = total
    each(XS, GROUP, lambda j: gather(j).start())
    each(1, XS, lambda j: gather(j).start())
    each(1, GROUP, lambda j: gather(j).wait_recv())

    R, Q, M, Y = (rh, rl), (qh, ql), (mh, ml), (yh, yl)

    def eye(x):
        rows = lax.broadcasted_iota(jnp.int32, x.shape, 0)
        cols = lax.broadcasted_iota(jnp.int32, x.shape, 1)
        return rows == cols

    def poly():
        m = COEF_C * product(R, R) + COEF_B * (rh[...].astype(F32) + rl[...].astype(F32))
        put(M, m + jnp.where(eye(m), COEF_A, 0.0))

    def advance():
        put(Y, product(M, R))
        put(R, product(Y, M))

    trace = jnp.zeros((), F32)
    for n, (i, j) in enumerate(PIECES):
        if i == j:
            part = full[128 * n : 128 * n + 128, :]
            trace = trace + jnp.sum(jnp.where(eye(part), part, 0.0))
    scale2 = trace + EPSILON
    inverse = 1.0 / jnp.full((1, 128), scale2, F32)
    for n, (i, j) in enumerate(PIECES):
        part = full[128 * n : 128 * n + 128, :] * inverse
        high, low = split(part)
        rows, cols = slice(128 * i, 128 * i + 128), slice(128 * j, 128 * j + 128)
        rh[rows, cols] = high
        rl[rows, cols] = low
        if i != j:
            high, low = split(part.T)
            rh[cols, rows] = high
            rl[cols, rows] = low
    def first_factor():
        qh[...] = mh[...]
        ql[...] = ml[...]

    def sweep(i):
        poly()
        pl.when(i == 0)(first_factor)
        pl.when(i > 0)(lambda: put(Q, product(Q, M)))
        advance()

    each(0, ITERS - 1, sweep)
    poly()
    factor[...] = (product(Q, M) * (1.0 / jnp.sqrt(jnp.full((1, ROWS), scale2, F32)))).astype(BF16)

    def strip(c):
        chip = lax.rem(z // 2 + c, ZS // 2)
        rows = pl.ds(pl.multiple_of(chip * 128, 128), 128)
        upd[rows, :] = (0.2 * math.sqrt(COLS) * dot(factor[rows, :], held[...])).astype(BF16)

        def send(i):
            dest = chip * 8 + i // 2
            b = lax.rem(i, 2)
            pl.when(jnp.logical_or(dest != me, b != core))(lambda: backward(b, dest).start())

        each(0, 16, send)

    each(0, ZS // 2, strip)
    keep_backward.start()
    keep_moment.wait()
    each(1, GROUP, lambda j: scatter(j).wait_send())
    each(1, GROUP, lambda j: gather(j).wait_send())
    others(lambda other, i: forward_in(other, i).wait_send())
    keep_backward.wait()
    others(lambda other, i: backward_in(other, i).wait_send())
    others(lambda other, i: backward_in(other, i).wait_recv())


def exchange(gradient, momentum):
    matrix = pltpu.VMEM((ROWS, ROWS), BF16)
    staged = pltpu.VMEM(gradient.shape, BF16)
    dma = pltpu.SemaphoreType.DMA
    return pl.pallas_call(
        kernel,
        out_shape=(
            jax.ShapeDtypeStruct((OUT, BLOCK, WIDTH), BF16),
            jax.ShapeDtypeStruct(momentum.shape, BF16),
        ),
        in_specs=[pl.BlockSpec(memory_space=pltpu.HBM)] * 2,
        out_specs=[pl.BlockSpec(memory_space=pl.ANY)] * 2,
        scratch_shapes=[
            pltpu.VMEM((OUT, BLOCK, WIDTH), BF16),
            pltpu.VMEM((ROWS, WIDTH), BF16),
            pltpu.VMEM((ROWS, WIDTH), BF16),
            pltpu.VMEM((TALL, 128), BF16),
            pltpu.VMEM((GROUP, SLICE, 128), BF16),
            pltpu.VMEM((SLICE, 128), F32),
            pltpu.VMEM((TALL, 128), F32),
            *[matrix] * 9,
            staged, staged, staged,
            dma((2, OUT)), dma((2, OUT)), dma((2, OUT)), dma((2, OUT)),
            dma((GROUP,)), dma((GROUP,)), dma((GROUP,)), dma((GROUP,)),
            dma((2,)), dma((2,)), dma,
        ],
        compiler_params=pltpu.CompilerParams(
            collective_id=0, has_side_effects=True, vmem_limit_bytes=VMEM_LIMIT
        ),
        name="muon",
    )(gradient, momentum)


def on_device(weight, gradient, momentum):
    returned, momentum_next = exchange(gradient, momentum)
    weight_next = 0.9 * weight - 0.5 * returned[:, :, : weight.shape[2]].astype(F32)
    return (weight_next, momentum_next)


def solution(mesh):
    spec = P(None, "out", "inp")
    return jax.shard_map(
        on_device, mesh=mesh, in_specs=(spec, spec, spec), out_specs=(spec, spec), check_vma=False
    )
```
